32 devices in a mesh: shard: 8 (over z, x), width: 4 (over y, core).
Axes of the slice: x: 2, y: 2, z: 4, core: 2. Of those that a mesh axis runs over, the one named last changes fastest.
Arguments:
- w_query: float32 [4096, 4096], P('shard', 'width'), may hold values from -0.125 to 0.125
- first_query: float32 [4096, 4096], P('shard', 'width'), may hold values from -0.09375 to 0.09375
- second_query: float32 [4096, 4096], P('shard', 'width'), may hold values from -0.09375 to 0.09375
- w_key: float32 [4096, 1024], P('shard', 'width'), may hold values from -0.125 to 0.125
- first_key: float32 [4096, 1024], P('shard', 'width'), may hold values from -0.09375 to 0.09375
- second_key: float32 [4096, 1024], P('shard', 'width'), may hold values from -0.09375 to 0.09375
- w_value: float32 [4096, 1024], P('shard', 'width'), may hold values from -0.125 to 0.125
- first_value: float32 [4096, 1024], P('shard', 'width'), may hold values from -0.09375 to 0.09375
- second_value: float32 [4096, 1024], P('shard', 'width'), may hold values from -0.09375 to 0.09375
- norm_train: float32 [4096], P(('shard', 'width')), may hold values from 0.25 to 1.75
- norm_step: float32 [4096], P(('shard', 'width')), may hold values from -0.3 to 0.3
Outputs:
- serving_query: bfloat16 [4096, 4096], P(None, 'width')
- serving_key: bfloat16 [4096, 1024], P(None, 'width')
- serving_value: bfloat16 [4096, 1024], P(None, 'width')
- column_query: float32 [4096], P('width')
- column_key: float32 [1024], P('width')
- column_value: float32 [1024], P('width')
- serve_norm: bfloat16 [4096], replicated
- whole_query: float32 [4096, 4096], P('shard', 'width')
- whole_key: float32 [4096, 1024], P('shard', 'width')
- whole_value: float32 [4096, 1024], P('shard', 'width')
The draws below stay inside these ranges and needn't reach their ends.
All inputs are finite; a program needn't handle non-finite values. Where the reference program divides by a largest or mean magnitude, that divisor is 1e-20 or more.
Results may differ from the reference program's by a relative error of at most 0.0004.
Values may be sent and summed in bfloat16 or wider, within the bound.
A program may use at most 128 MiB of HBM per device.

```python
import jax
import jax.numpy as jnp

D_MODEL = 4096
Q_DIM = 4096
KV_DIM = 1024


def raised(entries, stream_key, source, target, parts, factor):
    owner, partner = [(jnp.arange(entries.shape[dim]) // (entries.shape[dim] // parts)).reshape([-1 if axis == dim else 1 for axis in range(entries.ndim)]) for dim in (source, target)]
    chosen = jax.random.permutation(stream_key, parts)[partner]
    strong = (owner == chosen) | (owner == (partner + parts // 2) % parts)
    return jnp.where(strong, factor * entries, entries)


def block_levels(own_key, shape, pieces, least, high):
    loudness = 1.0
    for dim, parts in pieces:
        steps = jax.random.uniform(jax.random.fold_in(jax.random.fold_in(own_key, 6), dim), (parts,), jnp.float32, least / len(pieces), high / len(pieces))
        loudness = loudness * jnp.repeat(jnp.exp(steps), shape[dim] // parts).reshape((-1,) + (1,) * (len(shape) - 1 - dim))
    return loudness


def scatter_about(key, extent, spread, most, split=(), held_as=jnp.bfloat16):
    array = spread * jax.random.normal(key, extent, jnp.float32)
    if split:
        array = array * block_levels(key, extent, split, -0.22, 0.18)
    return jnp.clip(array, -most, most).astype(held_as)


def gaussian_with(stream_key, dims, deviation, reach, split, heavy, held_as=jnp.bfloat16):
    values = deviation * jax.random.normal(stream_key, dims, jnp.float32)
    if split:
        values = values * block_levels(stream_key, dims, split, -0.22, 0.18)
    return jnp.clip(raised(values, jax.random.fold_in(stream_key, 3), *heavy), -reach, reach).astype(held_as)


def setup_inputs(seed: int = 0) -> dict:
    seeds = jax.random.split(jax.random.key(seed), 12)
    return {
        "w_query": gaussian_with(seeds[0], (D_MODEL, Q_DIM), D_MODEL ** -0.5, 0.125, ((0, 8), (1, 4)), (0, 1, 8, 2.0), jnp.float32),
        "first_query": scatter_about(seeds[1], (D_MODEL, Q_DIM), D_MODEL ** -0.5, 0.09375, ((0, 8), (1, 4)), jnp.float32),
        "second_query": scatter_about(seeds[2], (D_MODEL, Q_DIM), D_MODEL ** -0.5, 0.09375, ((0, 8), (1, 4)), jnp.float32),
        "w_key": gaussian_with(seeds[3], (D_MODEL, KV_DIM), D_MODEL ** -0.5, 0.125, ((0, 8), (1, 4)), (0, 1, 8, 2.0), jnp.float32),
        "first_key": scatter_about(seeds[4], (D_MODEL, KV_DIM), D_MODEL ** -0.5, 0.09375, ((0, 8), (1, 4)), jnp.float32),
        "second_key": scatter_about(seeds[5], (D_MODEL, KV_DIM), D_MODEL ** -0.5, 0.09375, ((0, 8), (1, 4)), jnp.float32),
        "w_value": gaussian_with(seeds[6], (D_MODEL, KV_DIM), D_MODEL ** -0.5, 0.125, ((0, 8), (1, 4)), (0, 1, 8, 2.0), jnp.float32),
        "first_value": scatter_about(seeds[7], (D_MODEL, KV_DIM), D_MODEL ** -0.5, 0.09375, ((0, 8), (1, 4)), jnp.float32),
        "second_value": scatter_about(seeds[8], (D_MODEL, KV_DIM), D_MODEL ** -0.5, 0.09375, ((0, 8), (1, 4)), jnp.float32),
        "norm_train": jnp.clip(1.0 + 0.15 * jax.random.normal(seeds[9], (D_MODEL,), jnp.float32), 0.25, 1.75),
        "norm_step": jnp.clip(jax.random.uniform(seeds[10], (D_MODEL,), jnp.float32, -0.3, 0.3) * block_levels(seeds[10], (D_MODEL,), ((0, 32),), -0.4, 0.0), -0.3, 0.3),
    }


learn_rate = 0.2
hold_rate = 0.8


def reference(w_query, first_query, second_query, w_key, first_key, second_key, w_value, first_value, second_value, norm_train, norm_step):
    hold_query = hold_rate * first_query + second_query
    whole_query = w_query - learn_rate * hold_query
    hold_key = hold_rate * first_key + second_key
    whole_key = w_key - learn_rate * hold_key
    hold_value = hold_rate * first_value + second_value
    whole_value = w_value - learn_rate * hold_value
    column_query = jnp.sum(jnp.abs(whole_query), axis=0) / D_MODEL
    serving_query = (whole_query / column_query).astype(jnp.bfloat16)
    column_key = jnp.sum(jnp.abs(whole_key), axis=0) / D_MODEL
    serving_key = (whole_key / column_key).astype(jnp.bfloat16)
    column_value = jnp.sum(jnp.abs(whole_value), axis=0) / D_MODEL
    serving_value = (whole_value / column_value).astype(jnp.bfloat16)
    serve_norm = (norm_train + norm_step).astype(jnp.bfloat16)
    return serving_query, serving_key, serving_value, column_query, column_key, column_value, serve_norm, whole_query, whole_key, whole_value
```

```python
import functools

import jax
import jax.numpy as jnp
from jax import lax
from jax.experimental import pallas as pl
from jax.experimental.pallas import tpu as pltpu
from jax.sharding import PartitionSpec as P

learn_rate = 0.2
hold_rate = 0.8
MESH = pl.DeviceIdType.MESH
TILE = 16


def gather_kernel(
    n,
    width,
    w_q,
    w_k,
    w_v,
    norm_in,
    out_q,
    out_k,
    out_v,
    col_q,
    col_k,
    col_v,
    norm_out,
    sums,
    sum_send,
    sum_recv,
    wid_send,
    wid_recv,
    nrm_send,
    nrm_recv,
    z_send,
    z_recv,
    x_send,
    x_recv,
):
    me = lax.axis_index("shard")
    me_w = lax.axis_index("width")
    depth = n // 2
    z, x = lax.div(me, 2), lax.rem(me, 2)
    rows = w_q.shape[0]
    ins, outs, cols = (w_q, w_k, w_v), (out_q, out_k, out_v), (col_q, col_k, col_v)
    extents = [ref.shape[1] for ref in ins]
    starts = [sum(extents[:i]) for i in range(3)]

    barrier = pltpu.get_barrier_semaphore()
    for k in range(1, n):
        pl.semaphore_signal(
            barrier, inc=1, device_id={"shard": lax.rem(me + k, n)}, device_id_type=MESH
        )
    for k in range(1, width):
        pl.semaphore_signal(
            barrier, inc=1, device_id={"width": lax.rem(me_w + k, width)}, device_id_type=MESH
        )

    for ref, start, extent in zip(ins, starts, extents):

        def add(i, total, ref=ref):
            for j in range(4):
                total = total + jnp.abs(ref[pl.ds(pl.multiple_of(i * 32 + j * 8, 8), 8), :])
            return total

        total = lax.fori_loop(0, rows // 32, add, jnp.zeros((8, extent), jnp.float32))
        sums[me, :, start : start + extent] = jnp.sum(total, axis=0, keepdims=True)
    norm_out[me, me_w] = norm_in[...]

    pl.semaphore_wait(barrier, n - 1 + width - 1)

    sum_copies = []
    for k in range(1, n):
        copy = pltpu.make_async_remote_copy(
            src_ref=sums.at[me],
            dst_ref=sums.at[me],
            send_sem=sum_send.at[k - 1],
            recv_sem=sum_recv.at[k - 1],
            device_id={"shard": lax.rem(me + k, n)},
            device_id_type=MESH,
        )
        copy.start()
        sum_copies.append(copy)
    wid_copies = []
    for k in range(1, width):
        copy = pltpu.make_async_remote_copy(
            src_ref=norm_in,
            dst_ref=norm_out.at[me, me_w],
            send_sem=wid_send.at[k - 1],
            recv_sem=wid_recv.at[k - 1],
            device_id={"width": lax.rem(me_w + k, width)},
            device_id_type=MESH,
        )
        copy.start()
        wid_copies.append(copy)
    for copy in sum_copies:
        copy.wait_recv()

    for ref, out, col, start, extent in zip(ins, outs, cols, starts, extents):
        total = sums[0, :, start : start + extent]
        for k in range(1, n):
            total = total + sums[k, :, start : start + extent]
        col[...] = total / (rows * n)

    for ref, out, col in zip(ins, outs, cols):
        scale = col[...]

        def narrow(i, carry, ref=ref, out=out, scale=scale):
            here = pl.multiple_of(i * TILE, TILE)
            there = pl.multiple_of(me * rows + i * TILE, TILE)
            out[pl.ds(there, TILE), :] = (ref[pl.ds(here, TILE), :] / scale).astype(jnp.bfloat16)
            return carry

        lax.fori_loop(0, rows // TILE, narrow, 0)

    part_g = TILE * max(1, round(rows * 4 / 9 / (2 * TILE)))
    part_h = rows // 2 - part_g
    g_at = (0, part_g)
    h_at = (2 * part_g, 2 * part_g + part_h)
    started = []

    def send(owner, at, size, target, send_sems, recv_sems):
        copies = []
        where = pl.ds(pl.multiple_of(owner * rows + at, TILE), size)
        for i, out in enumerate(outs):
            copy = pltpu.make_async_remote_copy(
                src_ref=out.at[where],
                dst_ref=out.at[where],
                send_sem=send_sems.at[i],
                recv_sem=recv_sems.at[i],
                device_id={"shard": target},
                device_id_type=MESH,
            )
            copy.start()
            copies.append(copy)
        started.extend(copies)
        return copies

    def arrived(copies):
        for copy in copies:
            copy.wait_recv()

    other = z * 2 + 1 - x
    step_of = (1, depth - 1)
    next_of = [lax.rem(z + step_of[d], depth) * 2 + x for d in range(2)]

    def ring_send(kind, d, s):
        at_z = lax.rem(z + s * step_of[1 - d], depth)
        column = 1 - x if kind == 2 else x
        at, size = ((g_at[d], part_g), (h_at[d], part_h), (h_at[d], part_h))[kind]
        return send(
            at_z * 2 + column,
            at,
            size,
            next_of[d],
            z_send.at[d, kind, s],
            z_recv.at[d, kind, s],
        )

    def x_own(unit):
        at, size = ((h_at[0], part_h), (h_at[1], part_h), (g_at[0], part_g), (g_at[1], part_g))[unit]
        return send(me, at, size, other, x_send.at[unit], x_recv.at[unit])

    def x_forward(d, s):
        at_z = lax.rem(z + (s + 1) * step_of[1 - d], depth)
        unit = 4 + 2 * s + d
        return send(at_z * 2 + x, g_at[d], part_g, other, x_send.at[unit], x_recv.at[unit])

    ring = {}
    crossed = [x_own(0)]
    for d in range(2):
        ring[0, d, 0] = ring_send(0, d, 0)
    crossed.append(x_own(1))
    for d in range(2):
        ring[1, d, 0] = ring_send(1, d, 0)
    crossed.append(x_own(2))
    crossed.append(x_own(3))

    for copy in wid_copies:
        copy.wait_recv()
    nrm_copies = []
    for k in range(1, n):
        copy = pltpu.make_async_remote_copy(
            src_ref=norm_out.at[me],
            dst_ref=norm_out.at[me],
            send_sem=nrm_send.at[k - 1],
            recv_sem=nrm_recv.at[k - 1],
            device_id={"shard": lax.rem(me + k, n)},
            device_id_type=MESH,
        )
        copy.start()
        nrm_copies.append(copy)

    def ring_arrival(kind, s):
        for d in range(2):
            arrived(ring[kind, d, s])
            if s + 1 < depth - 1:
                ring[kind, d, s + 1] = ring_send(kind, d, s + 1)
            if kind == 0:
                crossed.append(x_forward(d, s))

    def cross_arrival(d):
        arrived(crossed[d])
        ring[2, d, 0] = ring_send(2, d, 0)

    ring_arrival(0, 0)
    cross_arrival(0)
    ring_arrival(1, 0)
    cross_arrival(1)
    for s in range(1, depth - 1):
        ring_arrival(0, s)
        ring_arrival(2, s - 1)
        ring_arrival(1, s)
    ring_arrival(2, depth - 2)
    for copies in crossed[2:]:
        arrived(copies)
    for copy in nrm_copies:
        copy.wait_recv()
    for copy in sum_copies + wid_copies + nrm_copies + started:
        copy.wait_send()


def local(
    n,
    width,
    w_query,
    first_query,
    second_query,
    w_key,
    first_key,
    second_key,
    w_value,
    first_value,
    second_value,
    norm_train,
    norm_step,
):
    whole_query = w_query - learn_rate * (hold_rate * first_query + second_query)
    whole_key = w_key - learn_rate * (hold_rate * first_key + second_key)
    whole_value = w_value - learn_rate * (hold_rate * first_value + second_value)
    norm = (norm_train + norm_step).reshape(1, -1)
    wholes = (whole_query, whole_key, whole_value)
    rows = whole_query.shape[0]
    extents = [each.shape[1] for each in wholes]
    piece = norm.shape[1]
    depth = n // 2
    dma = pltpu.SemaphoreType.DMA
    vmem = pl.BlockSpec(memory_space=pltpu.VMEM)
    gathered = pl.pallas_call(
        functools.partial(gather_kernel, n, width),
        out_shape=[jax.ShapeDtypeStruct((rows * n, e), jnp.bfloat16) for e in extents]
        + [jax.ShapeDtypeStruct((1, e), jnp.float32) for e in extents]
        + [jax.ShapeDtypeStruct((n, width, 1, piece), jnp.float32)],
        in_specs=[vmem] * 4,
        out_specs=[vmem] * 7,
        scratch_shapes=[
            pltpu.VMEM((n, 1, sum(extents)), jnp.float32),
            dma((n - 1,)),
            dma((n - 1,)),
            dma((width - 1,)),
            dma((width - 1,)),
            dma((n - 1,)),
            dma((n - 1,)),
            dma((2, 3, depth - 1, 3)),
            dma((2, 3, depth - 1, 3)),
            dma((4 + 2 * (depth - 1), 3)),
            dma((4 + 2 * (depth - 1), 3)),
        ],
        compiler_params=pltpu.CompilerParams(
            collective_id=0, has_side_effects=True, vmem_limit_bytes=48 * 1024 * 1024
        ),
    )(*wholes, norm)
    serving_query, serving_key, serving_value, column_query, column_key, column_value, gain = gathered
    return (
        serving_query,
        serving_key,
        serving_value,
        column_query.reshape(-1),
        column_key.reshape(-1),
        column_value.reshape(-1),
        gain.reshape(-1).astype(jnp.bfloat16),
        whole_query,
        whole_key,
        whole_value,
    )


def solution(mesh):
    split = P("shard", "width")
    both = P(("shard", "width"))
    n, width = mesh.shape["shard"], mesh.shape["width"]
    return jax.shard_map(
        functools.partial(local, n, width),
        mesh=mesh,
        in_specs=(split,) * 9 + (both, both),
        out_specs=(P(None, "width"),) * 3 + (P("width"),) * 3 + (P(),) + (split,) * 3,
        check_vma=False,
    )
```
